16 devices in a mesh: dp: 4 (over z, y), sp: 4 (over x, core).
Axes of the slice: x: 2, y: 2, z: 2, core: 2. Of those that a mesh axis runs over, the one named last changes fastest.
Arguments:
- latents: bfloat16 [16, 4, 1024, 1408], P('dp', 'sp'), parts along dimension 0
- text_ctx: bfloat16 [16, 256, 1408], P('dp'), parts along dimension 0
- modulation: float32 [16, 6, 1408], P('dp'), parts along dimension 0
- pos_temporal: float32 [4, 1408], replicated
- w_qkv_spatial: bfloat16 [3, 16, 88, 1408], replicated
- w_out_spatial: bfloat16 [16, 88, 1408], replicated
- w_qkv_temporal: bfloat16 [3, 16, 88, 1408], replicated
- w_out_temporal: bfloat16 [16, 88, 1408], replicated
- w_query_cross: bfloat16 [16, 88, 1408], replicated
- w_kv_cross: bfloat16 [2, 16, 88, 1408], replicated
- w_out_cross: bfloat16 [16, 88, 1408], replicated
- w_mlp_in: bfloat16 [1408, 5632], replicated
- w_mlp_out: bfloat16 [5632, 1408], replicated
Outputs:
- output: bfloat16 [16, 4, 1024, 1408], P('dp', 'sp'), parts along dimension 0
There are 4 independent parts. The reference program is written for one: setup_inputs(seed, part) draws one part's arguments, and reference() takes and returns one part's arrays. A program takes and returns all parts, laid end to end along the dimension named above; an argument that names none is the same for every part.
All inputs are finite; a program needn't handle non-finite values.
Results may differ from the reference program's by a relative error of at most 0.014981.
Values are sent between devices in bfloat16 or wider.
A program may use at most 1 GiB of HBM per device.

```python
import jax
import jax.numpy as jnp
from jax import lax

BATCH_SIZE = 4
NUM_FRAMES = 4
NUM_PATCHES = 1024
MODEL_WIDTH = 1408
NUM_HEADS = 16
TEXT_LEN = 256

HEAD_DIM = MODEL_WIDTH // NUM_HEADS
LN_EPS = 1e-6


def weight_draw(rng_key, arr_shape, fan_in):
    return (jax.random.normal(rng_key, arr_shape, jnp.float32) * (fan_in ** -0.5)).astype(jnp.bfloat16)


def setup_inputs(seed: int = 0, part: int = 0) -> dict:
    part_keys = jax.random.split(jax.random.fold_in(jax.random.key(seed), part), 6)
    shared_keys = jax.random.split(jax.random.key(seed + 1), 11)
    act_shape = (BATCH_SIZE, NUM_FRAMES, NUM_PATCHES, MODEL_WIDTH)
    token_base = jax.random.normal(part_keys[0], (BATCH_SIZE, 1, NUM_PATCHES, MODEL_WIDTH), jnp.float32)
    frame_base = jax.random.normal(part_keys[1], (BATCH_SIZE, NUM_FRAMES, 1, MODEL_WIDTH), jnp.float32)
    noise_part = jax.random.normal(part_keys[2], act_shape, jnp.float32)
    latents = (0.5 * token_base + 0.5 * frame_base + 0.6 * noise_part).astype(jnp.bfloat16)
    ctx_common = jax.random.normal(part_keys[3], (BATCH_SIZE, 1, MODEL_WIDTH), jnp.float32)
    ctx_noise = jax.random.normal(part_keys[4], (BATCH_SIZE, TEXT_LEN, MODEL_WIDTH), jnp.float32)
    text_ctx = (0.5 * ctx_common + ctx_noise).astype(jnp.bfloat16)
    gate_offset = jnp.array([0.0, 0.0, 1.0, 0.0, 0.0, 1.0], jnp.float32)[None, :, None]
    modulation = 0.3 * jax.random.normal(part_keys[5], (BATCH_SIZE, 6, MODEL_WIDTH), jnp.float32) + gate_offset
    pos_common = jax.random.normal(shared_keys[0], (1, MODEL_WIDTH), jnp.float32)
    pos_frames = jax.random.normal(shared_keys[1], (NUM_FRAMES, MODEL_WIDTH), jnp.float32)
    pos_temporal = 0.4 * pos_common + 0.4 * pos_frames
    head_shape = (NUM_HEADS, HEAD_DIM, MODEL_WIDTH)
    return {
        'latents': latents,
        'text_ctx': text_ctx,
        'modulation': modulation,
        'pos_temporal': pos_temporal,
        'w_qkv_spatial': weight_draw(shared_keys[2], (3,) + head_shape, MODEL_WIDTH),
        'w_out_spatial': weight_draw(shared_keys[3], head_shape, MODEL_WIDTH),
        'w_qkv_temporal': weight_draw(shared_keys[4], (3,) + head_shape, MODEL_WIDTH),
        'w_out_temporal': weight_draw(shared_keys[5], head_shape, MODEL_WIDTH),
        'w_query_cross': weight_draw(shared_keys[6], head_shape, MODEL_WIDTH),
        'w_kv_cross': weight_draw(shared_keys[7], (2,) + head_shape, MODEL_WIDTH),
        'w_out_cross': weight_draw(shared_keys[8], head_shape, MODEL_WIDTH),
        'w_mlp_in': weight_draw(shared_keys[9], (MODEL_WIDTH, 4 * MODEL_WIDTH), MODEL_WIDTH),
        'w_mlp_out': weight_draw(shared_keys[10], (4 * MODEL_WIDTH, MODEL_WIDTH), 4 * MODEL_WIDTH),
    }


def layer_norm(acts_in):
    centered = acts_in - jnp.mean(acts_in, axis=-1, keepdims=True)
    return centered * lax.rsqrt(jnp.mean(centered * centered, axis=-1, keepdims=True) + LN_EPS)


def attend(query_heads, key_heads, value_heads):
    scores = jnp.einsum('bqhd,bkhd->bhqk', query_heads.astype(jnp.float32), key_heads.astype(jnp.float32))
    attn_probs = jax.nn.softmax(scores * (HEAD_DIM ** -0.5), axis=-1).astype(jnp.bfloat16)
    mixed_out = jnp.einsum('bhqk,bkhd->bqhd', attn_probs.astype(jnp.float32), value_heads.astype(jnp.float32))
    return mixed_out.astype(jnp.bfloat16)


def qkv_proj(acts_in, weight):
    return jnp.einsum('bnc,jhdc->jbnhd', acts_in.astype(jnp.float32), weight.astype(jnp.float32)).astype(jnp.bfloat16)


def out_proj(mixed_in, weight):
    return jnp.einsum('bnhd,hdc->bnc', mixed_in.astype(jnp.float32), weight.astype(jnp.float32))


def reference(latents, text_ctx, modulation, pos_temporal, w_qkv_spatial, w_out_spatial, w_qkv_temporal, w_out_temporal, w_query_cross, w_kv_cross, w_out_cross, w_mlp_in, w_mlp_out):
    mod_rows = jnp.moveaxis(modulation, 1, 0)[:, :, None, :]

    def spatial_frame(frame_in):
        frame_f = frame_in.astype(jnp.float32)
        normed = (layer_norm(frame_f) * (1.0 + mod_rows[1]) + mod_rows[0]).astype(jnp.bfloat16)
        qkv_all = qkv_proj(normed, w_qkv_spatial)
        mixed_out = attend(qkv_all[0], qkv_all[1], qkv_all[2])
        return (frame_f + mod_rows[2] * out_proj(mixed_out, w_out_spatial)).astype(jnp.bfloat16)

    def temporal_patch(column_in):
        column_f = column_in.astype(jnp.float32)
        shifted = (column_f + pos_temporal[None]).astype(jnp.bfloat16)
        qkv_all = qkv_proj(shifted, w_qkv_temporal)
        mixed_out = attend(qkv_all[0], qkv_all[1], qkv_all[2])
        return (column_f + mod_rows[2] * out_proj(mixed_out, w_out_temporal)).astype(jnp.bfloat16)

    ctx_kv = qkv_proj(text_ctx, w_kv_cross)

    def cross_mlp_frame(frame_in):
        frame_f = frame_in.astype(jnp.float32)
        query_heads = qkv_proj(frame_in, w_query_cross[None])[0]
        mixed_out = attend(query_heads, ctx_kv[0], ctx_kv[1])
        after_cross = (frame_f + out_proj(mixed_out, w_out_cross)).astype(jnp.bfloat16)
        cross_f = after_cross.astype(jnp.float32)
        normed = (layer_norm(cross_f) * (1.0 + mod_rows[4]) + mod_rows[3]).astype(jnp.bfloat16)
        flat_rows = normed.reshape(-1, MODEL_WIDTH)
        mlp_hidden = jax.nn.gelu(jnp.dot(flat_rows, w_mlp_in, preferred_element_type=jnp.float32), approximate=True).astype(jnp.bfloat16)
        mlp_out = jnp.dot(mlp_hidden, w_mlp_out, preferred_element_type=jnp.float32).reshape(cross_f.shape)
        return (cross_f + mod_rows[5] * mlp_out).astype(jnp.bfloat16)

    after_spatial = lax.map(spatial_frame, jnp.moveaxis(latents, 1, 0))
    after_temporal = lax.map(temporal_patch, jnp.transpose(after_spatial, (2, 1, 0, 3)))
    out_frames = lax.map(cross_mlp_frame, jnp.transpose(after_temporal, (2, 1, 0, 3)))
    return jnp.moveaxis(out_frames, 0, 1)
```

```python
import functools

import jax
import jax.numpy as jnp
from jax import lax
from jax.experimental import pallas as pl
from jax.experimental.pallas import tpu as pltpu
from jax.sharding import PartitionSpec as P

LN_EPS = 1e-6
LOG2E = 1.4426950408889634
VMEM_LIMIT = 60 * 1024 * 1024
NT = (((1,), (1,)), ((), ()))
TN = (((0,), (0,)), ((), ()))
F32 = jnp.float32
BF16 = jnp.bfloat16


def dot(lhs, rhs, dims=(((1,), (0,)), ((), ()))):
    return lax.dot_general(lhs, rhs, dims, preferred_element_type=F32)


def normed_rows(rows, shift, scale):
    rows = rows.astype(F32)
    centered = rows - jnp.mean(rows, axis=-1, keepdims=True)
    unit = centered * lax.rsqrt(jnp.mean(centered * centered, axis=-1, keepdims=True) + LN_EPS)
    return (unit * (1.0 + scale) + shift).astype(BF16)


def resident(shape):
    return pl.BlockSpec(shape, lambda *_: (0,) * len(shape), pipeline_mode=pl.Buffered(1))


def project_heads(w_ref, acts, q_s, k_s, v_s, heads, dim, chunk):
    tokens = acts.shape[0]
    group = w_ref.shape[1]

    def body(i, carry):
        cols = pl.ds(pl.multiple_of(i * chunk, chunk), chunk)
        part = acts[cols, :]
        q_t = dot(w_ref[0], part, NT).reshape(heads, dim, chunk)
        q_s[:, :dim, cols] = q_t.astype(BF16)
        v_t = dot(w_ref[2], part, NT).reshape(heads, dim, chunk)
        v_s[:, :, cols] = v_t.astype(BF16)
        k_t = dot(w_ref[1], part, NT)
        for h in range(heads):
            k_s[h, cols, :dim] = k_t[h * dim:(h + 1) * dim].T.astype(BF16)
        return carry

    lax.fori_loop(0, tokens // chunk, body, 0)


def attend_block(k, v_t, q_t, scale):
    s = dot(k, q_t)
    p = jnp.exp2((s - jnp.max(s, axis=0, keepdims=True)) * scale)
    total = jnp.sum(p, axis=0, keepdims=True)
    return dot(v_t, p.astype(BF16)) / total


def spatial_kernel(me_ref, x_ref, mod_ref, w_ref, wo_hbm, o0, o1, o2, o3, u_s, q_s, k_s, v_s, a_s, wo_s, sem, *, heads, dim):
    g = pl.program_id(0)
    tokens = x_ref.shape[0]
    quarter = tokens // 4
    wo_copy = pltpu.make_async_copy(wo_hbm, wo_s, sem)
    scale = dim ** -0.5 * LOG2E

    @pl.when(g == 0)
    def _():
        wo_copy.start()
        q_s[:, dim:, :] = jnp.zeros((heads, q_s.shape[1] - dim, tokens), BF16)
        k_s[:, :, dim:] = jnp.zeros((heads, tokens, k_s.shape[2] - dim), BF16)

        def ln(i, carry):
            rows = pl.ds(pl.multiple_of(i * 128, 128), 128)
            u_s[rows, :] = normed_rows(x_ref[rows, :], mod_ref[0:1, :], mod_ref[1:2, :])
            return carry

        lax.fori_loop(0, tokens // 128, ln, 0)

    project_heads(w_ref, u_s, q_s, k_s, v_s, heads, dim, 512)

    def pair(i, carry):
        rows = pl.ds(pl.multiple_of((g * heads + 2 * i) * dim, 2 * dim), 2 * dim)
        for c in range(4):
            cols = slice(c * quarter, (c + 1) * quarter)
            outs = [attend_block(k_s[2 * i + h], v_s[2 * i + h], q_s[2 * i + h, :, cols], scale) for h in range(2)]
            a_s[rows, cols] = jnp.concatenate(outs, axis=0).astype(BF16)
        return carry

    lax.fori_loop(0, heads // 2, pair, 0)

    @pl.when(g == pl.num_programs(0) - 1)
    def _():
        wo_copy.wait()
        for d, o_ref in enumerate((o0, o1, o2, o3)):
            rows = pl.ds(pl.multiple_of(jnp.bitwise_xor(me_ref[0], d) * quarter, quarter), quarter)
            branch = dot(a_s[:, rows], wo_s[...], TN)
            o_ref[...] = (x_ref[rows, :].astype(F32) + mod_ref[2:3, :] * branch).astype(BF16)


def temporal_kernel(me_ref, x0, x1, x2, x3, mod_ref, pos_ref, w_ref, wo_hbm, o0, o1, o2, o3, z_s, q_s, k_s, v_s, a_s, wo_s, sem, *, heads, dim):
    g = pl.program_id(0)
    quarter = x0.shape[0]
    frames = (x0, x1, x2, x3)
    wo_copy = pltpu.make_async_copy(wo_hbm, wo_s, sem)
    scale = dim ** -0.5 * LOG2E

    @pl.when(g == 0)
    def _():
        wo_copy.start()
        for d, x in enumerate(frames):
            pos = pos_ref[pl.ds(jnp.bitwise_xor(me_ref[0], d), 1), :]
            z_s[d * quarter:(d + 1) * quarter, :] = (x[...].astype(F32) + pos).astype(BF16)

    def proj(i, carry):
        cols = pl.ds(pl.multiple_of(i * 512, 512), 512)
        part = z_s[cols, :]
        for j, dst in enumerate((q_s, k_s, v_s)):
            dst[:, :, cols] = dot(w_ref[j], part, NT).reshape(heads, dim, 512).astype(BF16)
        return carry

    lax.fori_loop(0, z_s.shape[0] // 512, proj, 0)

    def attend(h, cols):
        outs = []
        q = q_s[h].astype(F32)
        k = k_s[h].astype(F32)
        v = v_s[h].astype(F32)
        part = lambda a, t: a[:, t * quarter + cols:t * quarter + cols + 128]
        for tq in range(4):
            s = [jnp.sum(part(q, tq) * part(k, tk), axis=0, keepdims=True) for tk in range(4)]
            top = jnp.maximum(jnp.maximum(s[0], s[1]), jnp.maximum(s[2], s[3]))
            p = [jnp.exp2((one - top) * scale) for one in s]
            inv = 1.0 / (p[0] + p[1] + p[2] + p[3])
            p = [(one * inv).astype(BF16).astype(F32) for one in p]
            outs.append(p[0] * part(v, 0) + p[1] * part(v, 1) + p[2] * part(v, 2) + p[3] * part(v, 3))
        return outs

    def pair(i, carry):
        rows = pl.ds(pl.multiple_of((g * heads + 2 * i) * dim, 2 * dim), 2 * dim)
        for cols in range(0, quarter, 128):
            first = attend(2 * i, cols)
            second = attend(2 * i + 1, cols)
            for t in range(4):
                a_s[rows, t * quarter + cols:t * quarter + cols + 128] = jnp.concatenate([first[t], second[t]], axis=0).astype(BF16)
        return carry

    lax.fori_loop(0, heads // 2, pair, 0)

    @pl.when(g == pl.num_programs(0) - 1)
    def _():
        wo_copy.wait()
        for d, (x, o_ref) in enumerate(zip(frames, (o0, o1, o2, o3))):
            branch = dot(a_s[:, d * quarter:(d + 1) * quarter], wo_s[...], TN)
            o_ref[...] = (x[...].astype(F32) + mod_ref[2:3, :] * branch).astype(BF16)


def text_kernel(t_ref, w_ref, k_ref, v_ref, *, heads, dim):
    tokens = t_ref.shape[0]
    k_t = dot(w_ref[0], t_ref[...], NT)
    v_ref[...] = dot(w_ref[1], t_ref[...], NT).reshape(heads, dim, tokens).astype(BF16)
    for h in range(heads):
        k_ref[h] = k_t[h * dim:(h + 1) * dim].T.astype(BF16)


def cross_mlp_kernel(me_ref, x0, x1, x2, x3, mod_ref, k_ref, v_ref, wq_hbm, wo_hbm, w_in, w_out, *rest, heads, dim):
    y_ref, q_s, a_s, h_s, u_s, acc_s, wq_s, wo_s, sems = rest[-9:]
    step = pl.program_id(0)
    quarter = x0.shape[0]
    tokens = 4 * quarter
    scale = dim ** -0.5 * LOG2E

    @pl.when(step == 0)
    def _():
        q_copy = pltpu.make_async_copy(wq_hbm, wq_s, sems.at[0])
        o_copy = pltpu.make_async_copy(wo_hbm, wo_s, sems.at[1])
        q_copy.start()
        o_copy.start()
        q_copy.wait()
        for d, x in enumerate((x0, x1, x2, x3)):
            cols = slice(d * quarter, (d + 1) * quarter)
            q_s[:, :, cols] = dot(wq_s[...], x[...], NT).reshape(heads, dim, quarter).astype(BF16)

        def pair(i, carry):
            rows = pl.ds(pl.multiple_of(2 * i * dim, 2 * dim), 2 * dim)
            for d in range(4):
                cols = slice(d * quarter, (d + 1) * quarter)
                outs = [attend_block(k_ref[2 * i + h], v_ref[2 * i + h], q_s[2 * i + h, :, cols], scale) for h in range(2)]
                a_s[rows, cols] = jnp.concatenate(outs, axis=0).astype(BF16)
            return carry

        lax.fori_loop(0, heads // 2, pair, 0)
        o_copy.wait()
        for d, x in enumerate((x0, x1, x2, x3)):
            rows = slice(d * quarter, (d + 1) * quarter)
            branch = dot(a_s[:, rows], wo_s[...], TN)
            after = (x[...].astype(F32) + branch).astype(BF16)
            h_s[rows, :] = after
            u_s[rows, :] = normed_rows(after, mod_ref[3:4, :], mod_ref[4:5, :])

    def mlp(i, carry):
        rows = pl.ds(pl.multiple_of(i * 256, 256), 256)
        hidden = jax.nn.gelu(dot(u_s[rows, :], w_in[...]), approximate=True).astype(BF16)
        part = dot(hidden, w_out[...])

        @pl.when(step == 0)
        def _():
            acc_s[rows, :] = part

        @pl.when(step > 0)
        def _():
            acc_s[rows, :] += part

        return carry

    lax.fori_loop(0, tokens // 256, mlp, 0)

    @pl.when(step == pl.num_programs(0) - 1)
    def _():
        for d in range(4):
            rows = slice(d * quarter, (d + 1) * quarter)
            dst = pl.ds(pl.multiple_of(jnp.bitwise_xor(me_ref[0], d) * quarter, quarter), quarter)
            y_ref[dst, :] = (h_s[rows, :].astype(F32) + mod_ref[5:6, :] * acc_s[rows, :]).astype(BF16)


def cost(flops, nbytes, exps=0):
    return pl.CostEstimate(flops=int(flops), bytes_accessed=int(nbytes), transcendentals=int(exps))


def params():
    return pltpu.CompilerParams(dimension_semantics=("arbitrary",), vmem_limit_bytes=VMEM_LIMIT)


def spatial(me, latents, modulation, w_qkv, w_out, v, heads):
    tokens, width = latents.shape[2:]
    dim = w_qkv.shape[2]
    total = w_qkv.shape[1] * dim
    group, quarter = heads * dim, tokens // 4
    steps = w_qkv.shape[1] // heads
    spec = pltpu.PrefetchScalarGridSpec(
        num_scalar_prefetch=1,
        grid=(steps,),
        in_specs=[
            pl.BlockSpec((None, None, tokens, width), lambda g, me: (v, 0, 0, 0), pipeline_mode=pl.Buffered(1)),
            pl.BlockSpec((None, 6, width), lambda g, me: (v, 0, 0), pipeline_mode=pl.Buffered(1)),
            pl.BlockSpec((3, group, width), lambda g, me: (0, g, 0)),
            pl.BlockSpec(memory_space=pl.ANY),
        ],
        out_specs=[resident((quarter, width))] * 4,
        scratch_shapes=[
            pltpu.VMEM((tokens, width), BF16),
            pltpu.VMEM((heads, 128, tokens), BF16),
            pltpu.VMEM((heads, tokens, 128), BF16),
            pltpu.VMEM((heads, dim, tokens), BF16),
            pltpu.VMEM((total, tokens), BF16),
            pltpu.VMEM((total, width), BF16),
            pltpu.SemaphoreType.DMA,
        ],
    )
    return pl.pallas_call(
        functools.partial(spatial_kernel, heads=heads, dim=dim),
        grid_spec=spec,
        out_shape=[jax.ShapeDtypeStruct((quarter, width), BF16)] * 4,
        compiler_params=params(),
        cost_estimate=cost(2 * tokens * width * 4 * total + 4 * tokens * tokens * total, 2 * (4 * total * width + 2 * tokens * width), tokens * tokens * 16),
        name="spatial",
    )(me, latents, modulation, w_qkv.reshape(3, total, width), w_out.reshape(total, width))


def temporal(me, frames, modulation, pos, w_qkv, w_out, v, heads):
    quarter, width = frames[0].shape
    tokens = 4 * quarter
    dim = w_qkv.shape[2]
    total = w_qkv.shape[1] * dim
    group = heads * dim
    steps = w_qkv.shape[1] // heads
    spec = pltpu.PrefetchScalarGridSpec(
        num_scalar_prefetch=1,
        grid=(steps,),
        in_specs=[resident((quarter, width))] * 4 + [
            pl.BlockSpec((None, 6, width), lambda g, me: (v, 0, 0), pipeline_mode=pl.Buffered(1)),
            resident(pos.shape),
            pl.BlockSpec((3, group, width), lambda g, me: (0, g, 0)),
            pl.BlockSpec(memory_space=pl.ANY),
        ],
        out_specs=[resident((quarter, width))] * 4,
        scratch_shapes=[
            pltpu.VMEM((tokens, width), BF16),
            pltpu.VMEM((heads, dim, tokens), BF16),
            pltpu.VMEM((heads, dim, tokens), BF16),
            pltpu.VMEM((heads, dim, tokens), BF16),
            pltpu.VMEM((total, tokens), BF16),
            pltpu.VMEM((total, width), BF16),
            pltpu.SemaphoreType.DMA,
        ],
    )
    return pl.pallas_call(
        functools.partial(temporal_kernel, heads=heads, dim=dim),
        grid_spec=spec,
        out_shape=[jax.ShapeDtypeStruct((quarter, width), BF16)] * 4,
        compiler_params=params(),
        cost_estimate=cost(2 * tokens * width * 4 * total, 2 * (4 * total * width + 2 * tokens * width)),
        name="temporal",
    )(me, *frames, modulation, pos, w_qkv.reshape(3, total, width), w_out.reshape(total, width))


def text_kv(text, w_kv, heads):
    videos, length, width = text.shape
    dim = w_kv.shape[2]
    count = w_kv.shape[1]
    total = count * dim
    tokens = videos * length
    return pl.pallas_call(
        functools.partial(text_kernel, heads=heads, dim=dim),
        grid=(count // heads,),
        in_specs=[resident((tokens, width)), pl.BlockSpec((2, heads * dim, width), lambda g: (0, g, 0))],
        out_specs=[pl.BlockSpec((heads, tokens, dim), lambda g: (g, 0, 0)), pl.BlockSpec((heads, dim, tokens), lambda g: (g, 0, 0))],
        out_shape=[jax.ShapeDtypeStruct((count, tokens, dim), BF16), jax.ShapeDtypeStruct((count, dim, tokens), BF16)],
        compiler_params=params(),
        cost_estimate=cost(4 * tokens * width * total, 2 * (2 * total * width + 3 * tokens * width)),
        name="text_kv",
    )(text.reshape(tokens, width), w_kv.reshape(2, total, width))


def cross_mlp(me, chunks, modulation, k, v_t, w_query, w_out_cross, w_in, w_out, v, y, videos):
    quarter, width = chunks[0].shape
    tokens = 4 * quarter
    heads, all_text, dim = k.shape
    text = all_text // videos
    total = heads * dim
    hidden = w_in.shape[1]
    tile = 512
    steps = hidden // tile
    in_specs = [resident((quarter, width))] * 4 + [
        pl.BlockSpec((None, 6, width), lambda s, me: (v, 0, 0), pipeline_mode=pl.Buffered(1)),
        pl.BlockSpec((heads, text, dim), lambda s, me: (0, v, 0), pipeline_mode=pl.Buffered(1)),
        pl.BlockSpec((heads, dim, text), lambda s, me: (0, 0, v), pipeline_mode=pl.Buffered(1)),
        pl.BlockSpec(memory_space=pl.ANY),
        pl.BlockSpec(memory_space=pl.ANY),
        pl.BlockSpec((width, tile), lambda s, me: (0, s)),
        pl.BlockSpec((tile, width), lambda s, me: (s, 0)),
    ]
    args = [me, *chunks, modulation, k, v_t, w_query.reshape(total, width), w_out_cross.reshape(total, width), w_in, w_out]
    aliases = {}
    if y is not None:
        in_specs.append(pl.BlockSpec(memory_space=pl.ANY))
        aliases = {len(args): 0}
        args.append(y)
    spec = pltpu.PrefetchScalarGridSpec(
        num_scalar_prefetch=1,
        grid=(steps,),
        in_specs=in_specs,
        out_specs=pl.BlockSpec((None, None, tokens, width), lambda s, me: (v, 0, 0, 0), pipeline_mode=pl.Buffered(1)),
        scratch_shapes=[
            pltpu.VMEM((heads, dim, tokens), BF16),
            pltpu.VMEM((total, tokens), BF16),
            pltpu.VMEM((tokens, width), BF16),
            pltpu.VMEM((tokens, width), BF16),
            pltpu.VMEM((tokens, width), F32),
            pltpu.VMEM((total, width), BF16),
            pltpu.VMEM((total, width), BF16),
            pltpu.SemaphoreType.DMA((2,)),
        ],
    )
    return pl.pallas_call(
        functools.partial(cross_mlp_kernel, heads=heads, dim=dim),
        grid_spec=spec,
        out_shape=jax.ShapeDtypeStruct((videos, 1, tokens, width), BF16),
        input_output_aliases=aliases,
        compiler_params=params(),
        cost_estimate=cost(4 * tokens * width * (hidden + total) + 4 * tokens * text * total, 4 * (width * hidden + total * width + tokens * width)),
        name="cross_mlp",
    )(*args)


def swap(parts, devices):
    return [parts[0]] + [lax.ppermute(parts[d], 'sp', [(i, i ^ d) for i in range(devices)]) for d in range(1, devices)]


def solution(mesh):
    act_spec = P('dp', 'sp', None, None)
    row_spec = P('dp', None, None)
    rep_two = P(None, None)
    rep_three = P(None, None, None)
    rep_four = P(None, None, None, None)
    in_specs = (act_spec, row_spec, row_spec, rep_two, rep_four, rep_three, rep_four, rep_three, rep_three, rep_four, rep_three, rep_two, rep_two)
    devices = mesh.shape['sp']

    def local_block(latents, text_ctx, modulation, pos_temporal, w_qkv_spatial, w_out_spatial, w_qkv_temporal, w_out_temporal, w_query_cross, w_kv_cross, w_out_cross, w_mlp_in, w_mlp_out):
        videos = latents.shape[0]
        me = lax.axis_index('sp').astype(jnp.int32).reshape(1)
        by_patch = [swap(spatial(me, latents, modulation, w_qkv_spatial, w_out_spatial, v, 4), devices) for v in range(videos)]
        k, v_t = text_kv(text_ctx, w_kv_cross, 4)
        by_frame = [swap(temporal(me, by_patch[v], modulation, pos_temporal, w_qkv_temporal, w_out_temporal, v, 4), devices) for v in range(videos)]
        y = None
        for v in range(videos):
            y = cross_mlp(me, by_frame[v], modulation, k, v_t, w_query_cross, w_out_cross, w_mlp_in, w_mlp_out, v, y, videos)
        return y

    return jax.shard_map(local_block, mesh=mesh, in_specs=in_specs, out_specs=act_spec, check_vma=False)
```

```python
import functools

import jax
import jax.numpy as jnp
from jax import lax
from jax.experimental import pallas as pl
from jax.experimental.pallas import tpu as pltpu
from jax.sharding import PartitionSpec as P

LN_EPS = 1e-6
LOG2E = 1.4426950408889634
VMEM_LIMIT = 60 * 1024 * 1024
NT = (((1,), (1,)), ((), ()))
TN = (((0,), (0,)), ((), ()))
F32 = jnp.float32
BF16 = jnp.bfloat16


def dot(lhs, rhs, dims=(((1,), (0,)), ((), ()))):
    return lax.dot_general(lhs, rhs, dims, preferred_element_type=F32)


def normed_rows(rows, shift, scale):
    rows = rows.astype(F32)
    centered = rows - jnp.mean(rows, axis=-1, keepdims=True)
    unit = centered * lax.rsqrt(jnp.mean(centered * centered, axis=-1, keepdims=True) + LN_EPS)
    return (unit * (1.0 + scale) + shift).astype(BF16)


def resident(shape):
    return pl.BlockSpec(shape, lambda *_: (0,) * len(shape), pipeline_mode=pl.Buffered(1))


def project_heads(w_ref, acts, q_s, k_s, v_s, heads, dim, chunk):
    tokens = acts.shape[0]
    group = w_ref.shape[1]

    def body(i, carry):
        cols = pl.ds(pl.multiple_of(i * chunk, chunk), chunk)
        part = acts[cols, :]
        q_t = dot(w_ref[0], part, NT).reshape(heads, dim, chunk)
        q_s[:, :dim, cols] = q_t.astype(BF16)
        v_t = dot(w_ref[2], part, NT).reshape(heads, dim, chunk)
        v_s[:, :, cols] = v_t.astype(BF16)
        k_t = dot(w_ref[1], part, NT)
        for h in range(heads):
            k_s[h, cols, :dim] = k_t[h * dim:(h + 1) * dim].T.astype(BF16)
        return carry

    lax.fori_loop(0, tokens // chunk, body, 0)


def attend_heads(q, k, v, out, scores, probs, base, row, scale, count, block):
    tokens, keys, dim = out.shape[1], k.shape[1], v.shape[1]
    chunk = min(256, keys)
    blocks = [(h, c) for c in range(tokens // block) for h in range(count)]
    tops, mixed = {}, {}

    def score(n):
        h, c = blocks[n]
        top = None
        for r in range(0, keys, chunk):
            s = dot(k[base + h, r:r + chunk, :], q[base + h, :, c * block:(c + 1) * block])
            scores[n % 2][r:r + chunk, :] = s
            part = jnp.max(s.reshape(chunk // 8, 8, block), axis=0)
            top = part if top is None else jnp.maximum(top, part)
        tops[n] = jnp.max(top, axis=0, keepdims=True)

    def mix(n):
        h, c = blocks[n]
        total = None
        for r in range(0, keys, chunk):
            p = jnp.exp2((scores[n % 2][r:r + chunk, :] - tops[n]) * scale)
            part = jnp.sum(p.reshape(chunk // 8, 8, block), axis=0)
            total = part if total is None else total + part
            probs[n % 2][r:r + chunk, :] = p.astype(BF16)
        mixed[h] = dot(v[base + h], probs[n % 2][...]) / jnp.sum(total, axis=0, keepdims=True)
        if h == count - 1:
            out[pl.ds(row, count * dim), c * block:(c + 1) * block] = jnp.concatenate([mixed[i] for i in range(count)], axis=0).astype(BF16)

    score(0)
    for n in range(len(blocks)):
        if n + 1 < len(blocks):
            score(n + 1)
        mix(n)


def gelu(x):
    return x * (0.5 + 0.5 * jnp.tanh(x * (0.7978845608028654 + 0.7978845608028654 * 0.044715 * (x * x))))


def spatial_kernel(me_ref, x_ref, mod_ref, w_ref, wo_hbm, o0, o1, o2, o3, u_s, q_s, k_s, v_s, a_s, wo_s, s0, s1, p0, p1, sem, *, heads, dim):
    g = pl.program_id(0)
    tokens = x_ref.shape[0]
    quarter = tokens // 4
    wo_copy = pltpu.make_async_copy(wo_hbm, wo_s, sem)
    scale = dim ** -0.5 * LOG2E

    @pl.when(g == 0)
    def _():
        q_s[:, dim:, :] = jnp.zeros((heads, q_s.shape[1] - dim, tokens), BF16)
        k_s[:, :, dim:] = jnp.zeros((heads, tokens, k_s.shape[2] - dim), BF16)

        def ln(i, carry):
            rows = pl.ds(pl.multiple_of(i * 128, 128), 128)
            u_s[rows, :] = normed_rows(x_ref[rows, :], mod_ref[0:1, :], mod_ref[1:2, :])
            return carry

        lax.fori_loop(0, tokens // 128, ln, 0)

    project_heads(w_ref, u_s, q_s, k_s, v_s, heads, dim, 512)

    @pl.when(g == 1)
    def _():
        wo_copy.start()

    def pair(i, carry):
        row = pl.multiple_of((g * heads + 2 * i) * dim, 2 * dim)
        attend_heads(q_s, k_s, v_s, a_s, (s0, s1), (p0, p1), 2 * i, row, scale, 2, 512)
        return carry

    lax.fori_loop(0, heads // 2, pair, 0)

    @pl.when(g == pl.num_programs(0) - 1)
    def _():
        wo_copy.wait()
        for d, o_ref in enumerate((o0, o1, o2, o3)):
            rows = pl.ds(pl.multiple_of(jnp.bitwise_xor(me_ref[0], d) * quarter, quarter), quarter)
            branch = dot(a_s[:, rows], wo_s[...], TN)
            o_ref[...] = (x_ref[rows, :].astype(F32) + mod_ref[2:3, :] * branch).astype(BF16)


def temporal_kernel(me_ref, x0, x1, x2, x3, mod_ref, pos_ref, w_ref, wo_hbm, o0, o1, o2, o3, z_s, q_s, k_s, v_s, a_s, wo_s, sem, *, heads, dim):
    g = pl.program_id(0)
    quarter = x0.shape[0]
    frames = (x0, x1, x2, x3)
    wo_copy = pltpu.make_async_copy(wo_hbm, wo_s, sem)
    scale = dim ** -0.5 * LOG2E

    @pl.when(g == 0)
    def _():
        for d, x in enumerate(frames):
            pos = pos_ref[pl.ds(jnp.bitwise_xor(me_ref[0], d), 1), :]
            z_s[d * quarter:(d + 1) * quarter, :] = (x[...].astype(F32) + pos).astype(BF16)

    def proj(i, carry):
        cols = pl.ds(pl.multiple_of(i * 512, 512), 512)
        part = z_s[cols, :]
        for j, dst in enumerate((q_s, k_s, v_s)):
            dst[:, :, cols] = dot(w_ref[j], part, NT).reshape(heads, dim, 512).astype(BF16)
        return carry

    lax.fori_loop(0, z_s.shape[0] // 512, proj, 0)

    @pl.when(g == 1)
    def _():
        wo_copy.start()

    def attend(h, cols):
        outs = []
        q = q_s[h].astype(F32)
        k = k_s[h].astype(F32)
        v = v_s[h].astype(F32)
        part = lambda a, t: a[:, t * quarter + cols:t * quarter + cols + 128]
        for tq in range(4):
            s = [jnp.sum(part(q, tq) * part(k, tk), axis=0, keepdims=True) for tk in range(4)]
            top = jnp.maximum(jnp.maximum(s[0], s[1]), jnp.maximum(s[2], s[3]))
            p = [jnp.exp2((one - top) * scale) for one in s]
            inv = 1.0 / (p[0] + p[1] + p[2] + p[3])
            p = [(one * inv).astype(BF16).astype(F32) for one in p]
            outs.append(p[0] * part(v, 0) + p[1] * part(v, 1) + p[2] * part(v, 2) + p[3] * part(v, 3))
        return outs

    def pair(i, carry):
        rows = pl.ds(pl.multiple_of((g * heads + 2 * i) * dim, 2 * dim), 2 * dim)
        for cols in range(0, quarter, 128):
            first = attend(2 * i, cols)
            second = attend(2 * i + 1, cols)
            for t in range(4):
                a_s[rows, t * quarter + cols:t * quarter + cols + 128] = jnp.concatenate([first[t], second[t]], axis=0).astype(BF16)
        return carry

    lax.fori_loop(0, heads // 2, pair, 0)

    @pl.when(g == pl.num_programs(0) - 1)
    def _():
        wo_copy.wait()
        for d, (x, o_ref) in enumerate(zip(frames, (o0, o1, o2, o3))):
            branch = dot(a_s[:, d * quarter:(d + 1) * quarter], wo_s[...], TN)
            o_ref[...] = (x[...].astype(F32) + mod_ref[2:3, :] * branch).astype(BF16)


def text_kernel(t_ref, w_ref, k_ref, v_ref, *, heads, dim):
    tokens = t_ref.shape[0]
    k_t = dot(w_ref[0], t_ref[...], NT)
    v_ref[...] = dot(w_ref[1], t_ref[...], NT).reshape(heads, dim, tokens).astype(BF16)
    k_ref[:, :, dim:] = jnp.zeros((heads, tokens, k_ref.shape[2] - dim), BF16)
    for h in range(heads):
        k_ref[h, :, :dim] = k_t[h * dim:(h + 1) * dim].T.astype(BF16)


def cross_mlp_kernel(me_ref, x0, x1, x2, x3, mod_ref, k_ref, v_ref, wq_hbm, wo_hbm, w_in, w_out, *rest, heads, dim):
    y_ref, q_s, a_s, h_s, u_s, acc_s, wq_s, wo_s, s0, s1, p0, p1, sems = rest[-13:]
    step = pl.program_id(0)
    quarter = x0.shape[0]
    tokens = 4 * quarter
    scale = dim ** -0.5 * LOG2E

    @pl.when(step == 0)
    def _():
        acc_s[...] = jnp.zeros_like(acc_s)
        q_copy = pltpu.make_async_copy(wq_hbm, wq_s, sems.at[0])
        o_copy = pltpu.make_async_copy(wo_hbm, wo_s, sems.at[1])
        q_copy.start()
        o_copy.start()
        q_copy.wait()
        for d, x in enumerate((x0, x1, x2, x3)):
            cols = slice(d * quarter, (d + 1) * quarter)
            q_s[:, :dim, cols] = dot(wq_s[...], x[...], NT).reshape(heads, dim, quarter).astype(BF16)
        q_s[:, dim:, :] = jnp.zeros((heads, q_s.shape[1] - dim, tokens), BF16)

        def four(i, carry):
            row = pl.multiple_of(4 * i * dim, 4 * dim)
            attend_heads(q_s, k_ref, v_ref, a_s, (s0, s1), (p0, p1), 4 * i, row, scale, 4, 512)
            return carry

        lax.fori_loop(0, heads // 4, four, 0)
        o_copy.wait()
        for d, x in enumerate((x0, x1, x2, x3)):
            rows = slice(d * quarter, (d + 1) * quarter)
            branch = dot(a_s[:, rows], wo_s[...], TN)
            after = (x[...].astype(F32) + branch).astype(BF16)
            h_s[rows, :] = after
            u_s[rows, :] = normed_rows(after, mod_ref[3:4, :], mod_ref[4:5, :])

    hidden = gelu(dot(u_s[...], w_in[...])).astype(BF16)
    acc_s[...] += dot(hidden, w_out[...])

    @pl.when(step == pl.num_programs(0) - 1)
    def _():
        for d in range(4):
            rows = slice(d * quarter, (d + 1) * quarter)
            dst = pl.ds(pl.multiple_of(jnp.bitwise_xor(me_ref[0], d) * quarter, quarter), quarter)
            y_ref[dst, :] = (h_s[rows, :].astype(F32) + mod_ref[5:6, :] * acc_s[rows, :]).astype(BF16)


def cost(flops, nbytes, exps=0):
    return pl.CostEstimate(flops=int(flops), bytes_accessed=int(nbytes), transcendentals=int(exps))


def params():
    return pltpu.CompilerParams(dimension_semantics=("arbitrary",), vmem_limit_bytes=VMEM_LIMIT)


def spatial(me, latents, modulation, w_qkv, w_out, v, heads):
    tokens, width = latents.shape[2:]
    dim = w_qkv.shape[2]
    total = w_qkv.shape[1] * dim
    group, quarter = heads * dim, tokens // 4
    steps = w_qkv.shape[1] // heads
    spec = pltpu.PrefetchScalarGridSpec(
        num_scalar_prefetch=1,
        grid=(steps,),
        in_specs=[
            pl.BlockSpec((None, None, tokens, width), lambda g, me: (v, 0, 0, 0), pipeline_mode=pl.Buffered(1)),
            pl.BlockSpec((None, 6, width), lambda g, me: (v, 0, 0), pipeline_mode=pl.Buffered(1)),
            pl.BlockSpec((3, group, width), lambda g, me: (0, g, 0)),
            pl.BlockSpec(memory_space=pl.ANY),
        ],
        out_specs=[resident((quarter, width))] * 4,
        scratch_shapes=[
            pltpu.VMEM((tokens, width), BF16),
            pltpu.VMEM((heads, 128, tokens), BF16),
            pltpu.VMEM((heads, tokens, 128), BF16),
            pltpu.VMEM((heads, dim, tokens), BF16),
            pltpu.VMEM((total, tokens), BF16),
            pltpu.VMEM((total, width), BF16),
            pltpu.VMEM((tokens, 512), F32),
            pltpu.VMEM((tokens, 512), F32),
            pltpu.VMEM((tokens, 512), BF16),
            pltpu.VMEM((tokens, 512), BF16),
            pltpu.SemaphoreType.DMA,
        ],
    )
    return pl.pallas_call(
        functools.partial(spatial_kernel, heads=heads, dim=dim),
        grid_spec=spec,
        out_shape=[jax.ShapeDtypeStruct((quarter, width), BF16)] * 4,
        compiler_params=params(),
        cost_estimate=cost(2 * tokens * width * 4 * total + 4 * tokens * tokens * total, 2 * (4 * total * width + 2 * tokens * width), tokens * tokens * 16),
        name="spatial",
    )(me, latents, modulation, w_qkv.reshape(3, total, width), w_out.reshape(total, width))


def temporal(me, frames, modulation, pos, w_qkv, w_out, v, heads):
    quarter, width = frames[0].shape
    tokens = 4 * quarter
    dim = w_qkv.shape[2]
    total = w_qkv.shape[1] * dim
    group = heads * dim
    steps = w_qkv.shape[1] // heads
    spec = pltpu.PrefetchScalarGridSpec(
        num_scalar_prefetch=1,
        grid=(steps,),
        in_specs=[resident((quarter, width))] * 4 + [
            pl.BlockSpec((None, 6, width), lambda g, me: (v, 0, 0), pipeline_mode=pl.Buffered(1)),
            resident(pos.shape),
            pl.BlockSpec((3, group, width), lambda g, me: (0, g, 0)),
            pl.BlockSpec(memory_space=pl.ANY),
        ],
        out_specs=[resident((quarter, width))] * 4,
        scratch_shapes=[
            pltpu.VMEM((tokens, width), BF16),
            pltpu.VMEM((heads, dim, tokens), BF16),
            pltpu.VMEM((heads, dim, tokens), BF16),
            pltpu.VMEM((heads, dim, tokens), BF16),
            pltpu.VMEM((total, tokens), BF16),
            pltpu.VMEM((total, width), BF16),
            pltpu.SemaphoreType.DMA,
        ],
    )
    return pl.pallas_call(
        functools.partial(temporal_kernel, heads=heads, dim=dim),
        grid_spec=spec,
        out_shape=[jax.ShapeDtypeStruct((quarter, width), BF16)] * 4,
        compiler_params=params(),
        cost_estimate=cost(2 * tokens * width * 4 * total, 2 * (4 * total * width + 2 * tokens * width)),
        name="temporal",
    )(me, *frames, modulation, pos, w_qkv.reshape(3, total, width), w_out.reshape(total, width))


def text_kv(text, w_kv, heads):
    videos, length, width = text.shape
    dim = w_kv.shape[2]
    count = w_kv.shape[1]
    total = count * dim
    tokens = videos * length
    return pl.pallas_call(
        functools.partial(text_kernel, heads=heads, dim=dim),
        grid=(count // heads,),
        in_specs=[resident((tokens, width)), pl.BlockSpec((2, heads * dim, width), lambda g: (0, g, 0))],
        out_specs=[pl.BlockSpec((heads, tokens, 128), lambda g: (g, 0, 0)), pl.BlockSpec((heads, dim, tokens), lambda g: (g, 0, 0))],
        out_shape=[jax.ShapeDtypeStruct((count, tokens, 128), BF16), jax.ShapeDtypeStruct((count, dim, tokens), BF16)],
        compiler_params=params(),
        cost_estimate=cost(4 * tokens * width * total, 2 * (2 * total * width + 3 * tokens * width)),
        name="text_kv",
    )(text.reshape(tokens, width), w_kv.reshape(2, total, width))


def cross_mlp(me, chunks, modulation, k, v_t, w_query, w_out_cross, w_in, w_out, v, y, videos):
    quarter, width = chunks[0].shape
    tokens = 4 * quarter
    heads, dim, all_text = v_t.shape
    text = all_text // videos
    total = heads * dim
    hidden = w_in.shape[1]
    tile = 512
    steps = hidden // tile
    in_specs = [resident((quarter, width))] * 4 + [
        pl.BlockSpec((None, 6, width), lambda s, me: (v, 0, 0), pipeline_mode=pl.Buffered(1)),
        pl.BlockSpec((heads, text, k.shape[2]), lambda s, me: (0, v, 0), pipeline_mode=pl.Buffered(1)),
        pl.BlockSpec((heads, dim, text), lambda s, me: (0, 0, v), pipeline_mode=pl.Buffered(1)),
        pl.BlockSpec(memory_space=pl.ANY),
        pl.BlockSpec(memory_space=pl.ANY),
        pl.BlockSpec((width, tile), lambda s, me: (0, s)),
        pl.BlockSpec((tile, width), lambda s, me: (s, 0)),
    ]
    args = [me, *chunks, modulation, k, v_t, w_query.reshape(total, width), w_out_cross.reshape(total, width), w_in, w_out]
    aliases = {}
    if y is not None:
        in_specs.append(pl.BlockSpec(memory_space=pl.ANY))
        aliases = {len(args): 0}
        args.append(y)
    spec = pltpu.PrefetchScalarGridSpec(
        num_scalar_prefetch=1,
        grid=(steps,),
        in_specs=in_specs,
        out_specs=pl.BlockSpec((None, None, tokens, width), lambda s, me: (v, 0, 0, 0), pipeline_mode=pl.Buffered(1)),
        scratch_shapes=[
            pltpu.VMEM((heads, 128, tokens), BF16),
            pltpu.VMEM((total, tokens), BF16),
            pltpu.VMEM((tokens, width), BF16),
            pltpu.VMEM((tokens, width), BF16),
            pltpu.VMEM((tokens, width), F32),
            pltpu.VMEM((total, width), BF16),
            pltpu.VMEM((total, width), BF16),
            pltpu.VMEM((text, 512), F32),
            pltpu.VMEM((text, 512), F32),
            pltpu.VMEM((text, 512), BF16),
            pltpu.VMEM((text, 512), BF16),
            pltpu.SemaphoreType.DMA((2,)),
        ],
    )
    return pl.pallas_call(
        functools.partial(cross_mlp_kernel, heads=heads, dim=dim),
        grid_spec=spec,
        out_shape=jax.ShapeDtypeStruct((videos, 1, tokens, width), BF16),
        input_output_aliases=aliases,
        compiler_params=params(),
        cost_estimate=cost(4 * tokens * width * (hidden + total) + 4 * tokens * text * total, 4 * (width * hidden + total * width + tokens * width)),
        name="cross_mlp",
    )(*args)


def swap(parts, devices):
    return [parts[0]] + [lax.ppermute(parts[d], 'sp', [(i, i ^ d) for i in range(devices)]) for d in range(1, devices)]


def solution(mesh):
    act_spec = P('dp', 'sp', None, None)
    row_spec = P('dp', None, None)
    rep_two = P(None, None)
    rep_three = P(None, None, None)
    rep_four = P(None, None, None, None)
    in_specs = (act_spec, row_spec, row_spec, rep_two, rep_four, rep_three, rep_four, rep_three, rep_three, rep_four, rep_three, rep_two, rep_two)
    devices = mesh.shape['sp']

    def local_block(latents, text_ctx, modulation, pos_temporal, w_qkv_spatial, w_out_spatial, w_qkv_temporal, w_out_temporal, w_query_cross, w_kv_cross, w_out_cross, w_mlp_in, w_mlp_out):
        videos = latents.shape[0]
        me = lax.axis_index('sp').astype(jnp.int32).reshape(1)
        by_patch = [swap(spatial(me, latents, modulation, w_qkv_spatial, w_out_spatial, v, 4), devices) for v in range(videos)]
        k, v_t = text_kv(text_ctx, w_kv_cross, 4)
        by_frame = [swap(temporal(me, by_patch[v], modulation, pos_temporal, w_qkv_temporal, w_out_temporal, v, 4), devices) for v in range(videos)]
        y = None
        for v in range(videos):
            y = cross_mlp(me, by_frame[v], modulation, k, v_t, w_query_cross, w_out_cross, w_mlp_in, w_mlp_out, v, y, videos)
        return y

    return jax.shard_map(local_block, mesh=mesh, in_specs=in_specs, out_specs=act_spec, check_vma=False)
```

```python
import functools

import jax
import jax.numpy as jnp
from jax import lax
from jax.experimental import pallas as pl
from jax.experimental.pallas import tpu as pltpu
from jax.sharding import PartitionSpec as P

LN_EPS = 1e-6
LOG2E = 1.4426950408889634
VMEM_LIMIT = 60 * 1024 * 1024
NT = (((1,), (1,)), ((), ()))
TN = (((0,), (0,)), ((), ()))
F32 = jnp.float32
BF16 = jnp.bfloat16


def dot(lhs, rhs, dims=(((1,), (0,)), ((), ()))):
    return lax.dot_general(lhs, rhs, dims, preferred_element_type=F32)


def normed_rows(rows, shift, scale):
    rows = rows.astype(F32)
    centered = rows - jnp.mean(rows, axis=-1, keepdims=True)
    unit = centered * lax.rsqrt(jnp.mean(centered * centered, axis=-1, keepdims=True) + LN_EPS)
    return (unit * (1.0 + scale) + shift).astype(BF16)


def resident(shape):
    return pl.BlockSpec(shape, lambda *_: (0,) * len(shape), pipeline_mode=pl.Buffered(1))


def project_heads(w_ref, acts, q_s, k_s, v_s, heads, dim, cols):
    chunk = cols.stop - cols.start
    part = acts[cols, :]
    q_s[:, :dim, cols] = dot(w_ref[0], part, NT).reshape(heads, dim, chunk).astype(BF16)
    v_s[:, :, cols] = dot(w_ref[2], part, NT).reshape(heads, dim, chunk).astype(BF16)
    k_t = dot(w_ref[1], part, NT)
    for h in range(heads):
        k_s[h, cols, :dim] = k_t[h * dim:(h + 1) * dim].T.astype(BF16)


def attend_heads(q, k, v, out, scores, probs, base, row, scale, count, block):
    tokens, keys, dim = out.shape[1], k.shape[1], v.shape[1]
    chunk = min(256, keys)
    blocks = [(h, c) for c in range(tokens // block) for h in range(count)]
    tops, mixed = {}, {}

    def score(n):
        h, c = blocks[n]
        top = None
        for r in range(0, keys, chunk):
            s = dot(k[base + h, r:r + chunk, :], q[base + h, :, c * block:(c + 1) * block])
            scores[n % 2][r:r + chunk, :] = s
            part = jnp.max(s.reshape(chunk // 8, 8, block), axis=0)
            top = part if top is None else jnp.maximum(top, part)
        tops[n] = jnp.max(top, axis=0, keepdims=True)

    def mix(n):
        h, c = blocks[n]
        total = None
        for r in range(0, keys, chunk):
            p = jnp.exp2((scores[n % 2][r:r + chunk, :] - tops[n]) * scale)
            part = jnp.sum(p.reshape(chunk // 8, 8, block), axis=0)
            total = part if total is None else total + part
            probs[n % 2][r:r + chunk, :] = p.astype(BF16)
        mixed[h] = dot(v[base + h], probs[n % 2][...]) / jnp.sum(total, axis=0, keepdims=True)
        if h == count - 1:
            out[pl.ds(row, count * dim), c * block:(c + 1) * block] = jnp.concatenate([mixed[i] for i in range(count)], axis=0).astype(BF16)

    score(0)
    for n in range(len(blocks)):
        if n + 1 < len(blocks):
            score(n + 1)
        mix(n)


def gelu(x):
    return x * (0.5 + 0.5 * jnp.tanh(x * (0.7978845608028654 + 0.7978845608028654 * 0.044715 * (x * x))))


def spatial_kernel(me_ref, x_ref, mod_ref, w_ref, wo_hbm, o0, o1, o2, o3, u_s, q_s, k_s, v_s, a_s, wo_s, s0, s1, p0, p1, sem, *, heads, dim):
    v, g = pl.program_id(0), pl.program_id(1)
    tokens = x_ref.shape[0]
    quarter = tokens // 4
    halves = (slice(0, tokens // 2), slice(tokens // 2, tokens))
    wo_copy = pltpu.make_async_copy(wo_hbm, wo_s, sem)
    scale = dim ** -0.5 * LOG2E

    @pl.when((v == 0) & (g == 0))
    def _():
        q_s[:, dim:, :] = jnp.zeros((heads, q_s.shape[1] - dim, tokens), BF16)
        k_s[:, :, dim:] = jnp.zeros((heads, tokens, k_s.shape[2] - dim), BF16)

    @pl.when(g == 0)
    def _():
        for rows in halves:
            u_s[rows, :] = normed_rows(x_ref[rows, :], mod_ref[0:1, :], mod_ref[1:2, :])
            project_heads(w_ref, u_s, q_s, k_s, v_s, heads, dim, rows)

    @pl.when(g > 0)
    def _():
        for rows in halves:
            project_heads(w_ref, u_s, q_s, k_s, v_s, heads, dim, rows)

    @pl.when((v == 0) & (g == 1))
    def _():
        wo_copy.start()

    def pair(i, carry):
        row = pl.multiple_of((g * heads + 2 * i) * dim, 2 * dim)
        attend_heads(q_s, k_s, v_s, a_s, (s0, s1), (p0, p1), 2 * i, row, scale, 2, 512)
        return carry

    lax.fori_loop(0, heads // 2, pair, 0)

    @pl.when((v == 0) & (g == pl.num_programs(1) - 1))
    def _():
        wo_copy.wait()

    @pl.when(g == pl.num_programs(1) - 1)
    def _():
        for d, o_ref in enumerate((o0, o1, o2, o3)):
            rows = pl.ds(pl.multiple_of(jnp.bitwise_xor(me_ref[0], d) * quarter, quarter), quarter)
            branch = dot(a_s[:, rows], wo_s[...], TN)
            o_ref[...] = (x_ref[rows, :].astype(F32) + mod_ref[2:3, :] * branch).astype(BF16)


def attend_frames(q_s, k_s, v_s, h, cols, quarter, scale):
    part = lambda ref, t: ref[h, :, t * quarter + cols:t * quarter + cols + 128].astype(F32)
    k = [part(k_s, t) for t in range(4)]
    v = [part(v_s, t) for t in range(4)]
    outs = []
    for t in range(4):
        q = part(q_s, t)
        s = [jnp.sum(q * one, axis=0, keepdims=True) for one in k]
        top = jnp.maximum(jnp.maximum(s[0], s[1]), jnp.maximum(s[2], s[3]))
        p = [jnp.exp2((one - top) * scale) for one in s]
        inv = 1.0 / (p[0] + p[1] + p[2] + p[3])
        p = [(one * inv).astype(BF16).astype(F32) for one in p]
        outs.append(p[0] * v[0] + p[1] * v[1] + p[2] * v[2] + p[3] * v[3])
    return outs


def temporal_kernel(me_ref, x0, x1, x2, x3, mod_ref, pos_ref, w_ref, wo_hbm, o0, o1, o2, o3, z_s, qa, ka, va, qb, kb, vb, a_s, wo_s, sem, *, heads, dim):
    v, g = pl.program_id(0), pl.program_id(1)
    quarter = x0.shape[0]
    frames = (x0, x1, x2, x3)
    group = heads * dim
    wo_copy = pltpu.make_async_copy(wo_hbm, wo_s, sem)
    scale = dim ** -0.5 * LOG2E

    def shift(d):
        pos = pos_ref[pl.ds(jnp.bitwise_xor(me_ref[0], d), 1), :]
        z_s[d * quarter:(d + 1) * quarter, :] = (frames[d][...].astype(F32) + pos).astype(BF16)

    def project(half, dsts, tokens):
        for j, dst in enumerate(dsts):
            part = dot(w_ref[j, half * group:(half + 1) * group, :], z_s[tokens, :], NT)
            dst[:, :, tokens] = part.reshape(heads, dim, 2 * quarter).astype(BF16)

    def attend(srcs, index):
        for i in range(heads // 2):
            rows = pl.ds(pl.multiple_of(index * group + 2 * i * dim, 2 * dim), 2 * dim)
            for cols in range(0, quarter, 128):
                first = attend_frames(*srcs, 2 * i, cols, quarter, scale)
                second = attend_frames(*srcs, 2 * i + 1, cols, quarter, scale)
                for t in range(4):
                    out = jnp.concatenate([first[t], second[t]], axis=0)
                    a_s[rows, t * quarter + cols:t * quarter + cols + 128] = out.astype(BF16)

    halves = (slice(0, 2 * quarter), slice(2 * quarter, 4 * quarter))
    first, second = (qa, ka, va), (qb, kb, vb)

    @pl.when(g == 0)
    def _():
        for d in range(4):
            shift(d)
        for tokens in halves:
            project(0, first, tokens)

    @pl.when(g > 0)
    def _():
        for tokens in halves:
            project(0, first, tokens)
        attend(second, 2 * g - 1)

    for tokens in halves:
        project(1, second, tokens)
    attend(first, 2 * g)

    @pl.when((v == 0) & (g == 0))
    def _():
        wo_copy.start()

    @pl.when((v == 0) & (g == pl.num_programs(1) - 1))
    def _():
        wo_copy.wait()

    @pl.when(g == pl.num_programs(1) - 1)
    def _():
        attend(second, 2 * g + 1)
        for d, (x, o_ref) in enumerate(zip(frames, (o0, o1, o2, o3))):
            branch = dot(a_s[:, d * quarter:(d + 1) * quarter], wo_s[...], TN)
            o_ref[...] = (x[...].astype(F32) + mod_ref[2:3, :] * branch).astype(BF16)


def text_kernel(t_ref, w_ref, k_ref, v_ref, *, heads, dim):
    tokens = t_ref.shape[0]
    k_t = dot(w_ref[0], t_ref[...], NT)
    v_ref[...] = dot(w_ref[1], t_ref[...], NT).reshape(heads, dim, tokens).astype(BF16)
    k_ref[:, :, dim:] = jnp.zeros((heads, tokens, k_ref.shape[2] - dim), BF16)
    for h in range(heads):
        k_ref[h, :, :dim] = k_t[h * dim:(h + 1) * dim].T.astype(BF16)


def cross_mlp_kernel(me_ref, x0, x1, x2, x3, mod_ref, k_ref, v_ref, wq_hbm, wo_hbm, w_in, w_out, *rest, heads, dim):
    y_ref, q_s, a_s, h_s, u_s, acc_s, wq_s, wo_s, s0, s1, p0, p1, sems = rest[-13:]
    v, step = pl.program_id(0), pl.program_id(1)
    quarter = x0.shape[0]
    tokens = 4 * quarter
    scale = dim ** -0.5 * LOG2E

    @pl.when(step == 0)
    def _():
        acc_s[...] = jnp.zeros_like(acc_s)

        @pl.when(v == 0)
        def _():
            pltpu.make_async_copy(wq_hbm, wq_s, sems.at[0]).start()
            pltpu.make_async_copy(wq_hbm, wq_s, sems.at[0]).wait()
            pltpu.make_async_copy(wo_hbm, wo_s, sems.at[1]).start()

        for d, x in enumerate((x0, x1, x2, x3)):
            cols = slice(d * quarter, (d + 1) * quarter)
            q_s[:, :dim, cols] = dot(wq_s[...], x[...], NT).reshape(heads, dim, quarter).astype(BF16)
        q_s[:, dim:, :] = jnp.zeros((heads, q_s.shape[1] - dim, tokens), BF16)

        def four(i, carry):
            row = pl.multiple_of(4 * i * dim, 4 * dim)
            attend_heads(q_s, k_ref, v_ref, a_s, (s0, s1), (p0, p1), 4 * i, row, scale, 4, 512)
            return carry

        lax.fori_loop(0, heads // 4, four, 0)

        @pl.when(v == 0)
        def _():
            pltpu.make_async_copy(wo_hbm, wo_s, sems.at[1]).wait()

        for d, x in enumerate((x0, x1, x2, x3)):
            rows = slice(d * quarter, (d + 1) * quarter)
            branch = dot(a_s[:, rows], wo_s[...], TN)
            after = (x[...].astype(F32) + branch).astype(BF16)
            h_s[rows, :] = after
            u_s[rows, :] = normed_rows(after, mod_ref[3:4, :], mod_ref[4:5, :])

    hidden = gelu(dot(u_s[...], w_in[...])).astype(BF16)
    acc_s[...] += dot(hidden, w_out[...])

    @pl.when(step == pl.num_programs(1) - 1)
    def _():
        for d in range(4):
            rows = slice(d * quarter, (d + 1) * quarter)
            dst = pl.ds(pl.multiple_of(jnp.bitwise_xor(me_ref[0], d) * quarter, quarter), quarter)
            y_ref[dst, :] = (h_s[rows, :].astype(F32) + mod_ref[5:6, :] * acc_s[rows, :]).astype(BF16)


def cost(flops, nbytes, exps=0):
    return pl.CostEstimate(flops=int(flops), bytes_accessed=int(nbytes), transcendentals=int(exps))


def params(axes=2):
    return pltpu.CompilerParams(dimension_semantics=("arbitrary",) * axes, vmem_limit_bytes=VMEM_LIMIT)


def spatial(me, latents, modulation, w_qkv, w_out, base, videos, heads):
    tokens, width = latents.shape[2:]
    dim = w_qkv.shape[2]
    total = w_qkv.shape[1] * dim
    group, quarter = heads * dim, tokens // 4
    spec = pltpu.PrefetchScalarGridSpec(
        num_scalar_prefetch=1,
        grid=(videos, w_qkv.shape[1] // heads),
        in_specs=[
            pl.BlockSpec((None, None, tokens, width), lambda v, g, me: (base + v, 0, 0, 0)),
            pl.BlockSpec((None, 6, width), lambda v, g, me: (base + v, 0, 0)),
            pl.BlockSpec((3, group, width), lambda v, g, me: (0, g, 0)),
            pl.BlockSpec(memory_space=pl.ANY),
        ],
        out_specs=[pl.BlockSpec((None, quarter, width), lambda v, g, me: (v, 0, 0))] * 4,
        scratch_shapes=[
            pltpu.VMEM((tokens, width), BF16),
            pltpu.VMEM((heads, 128, tokens), BF16),
            pltpu.VMEM((heads, tokens, 128), BF16),
            pltpu.VMEM((heads, dim, tokens), BF16),
            pltpu.VMEM((total, tokens), BF16),
            pltpu.VMEM((total, width), BF16),
            pltpu.VMEM((tokens, 512), F32),
            pltpu.VMEM((tokens, 512), F32),
            pltpu.VMEM((tokens, 512), BF16),
            pltpu.VMEM((tokens, 512), BF16),
            pltpu.SemaphoreType.DMA,
        ],
    )
    return pl.pallas_call(
        functools.partial(spatial_kernel, heads=heads, dim=dim),
        grid_spec=spec,
        out_shape=[jax.ShapeDtypeStruct((videos, quarter, width), BF16)] * 4,
        compiler_params=params(),
        cost_estimate=cost(videos * (8 * tokens * width * total + 4 * tokens * tokens * total), 2 * (4 * total * width + 2 * videos * tokens * width)),
        name="spatial",
    )(me, latents, modulation, w_qkv.reshape(3, total, width), w_out.reshape(total, width))


def temporal(me, frames, modulation, pos, w_qkv, w_out, base, heads):
    videos, quarter, width = frames[0].shape
    tokens = 4 * quarter
    dim = w_qkv.shape[2]
    total = w_qkv.shape[1] * dim
    group = heads * dim
    spec = pltpu.PrefetchScalarGridSpec(
        num_scalar_prefetch=1,
        grid=(videos, w_qkv.shape[1] // (2 * heads)),
        in_specs=[pl.BlockSpec((None, quarter, width), lambda v, g, me: (v, 0, 0))] * 4 + [
            pl.BlockSpec((None, 6, width), lambda v, g, me: (base + v, 0, 0)),
            resident(pos.shape),
            pl.BlockSpec((3, 2 * group, width), lambda v, g, me: (0, g, 0)),
            pl.BlockSpec(memory_space=pl.ANY),
        ],
        out_specs=[pl.BlockSpec((None, quarter, width), lambda v, g, me: (v, 0, 0))] * 4,
        scratch_shapes=[pltpu.VMEM((tokens, width), BF16)] + [pltpu.VMEM((heads, dim, tokens), BF16)] * 6 + [
            pltpu.VMEM((total, tokens), BF16),
            pltpu.VMEM((total, width), BF16),
            pltpu.SemaphoreType.DMA,
        ],
    )
    return pl.pallas_call(
        functools.partial(temporal_kernel, heads=heads, dim=dim),
        grid_spec=spec,
        out_shape=[jax.ShapeDtypeStruct((videos, quarter, width), BF16)] * 4,
        compiler_params=params(),
        cost_estimate=cost(videos * 8 * tokens * width * total, 2 * (4 * total * width + 2 * videos * tokens * width)),
        name="temporal",
    )(me, *frames, modulation, pos, w_qkv.reshape(3, total, width), w_out.reshape(total, width))


def text_kv(text, w_kv, heads):
    videos, length, width = text.shape
    dim = w_kv.shape[2]
    count = w_kv.shape[1]
    total = count * dim
    tokens = videos * length
    return pl.pallas_call(
        functools.partial(text_kernel, heads=heads, dim=dim),
        grid=(count // heads,),
        in_specs=[resident((tokens, width)), pl.BlockSpec((2, heads * dim, width), lambda g: (0, g, 0))],
        out_specs=[pl.BlockSpec((heads, tokens, 128), lambda g: (g, 0, 0)), pl.BlockSpec((heads, dim, tokens), lambda g: (g, 0, 0))],
        out_shape=[jax.ShapeDtypeStruct((count, tokens, 128), BF16), jax.ShapeDtypeStruct((count, dim, tokens), BF16)],
        compiler_params=params(1),
        cost_estimate=cost(4 * tokens * width * total, 2 * (2 * total * width + 3 * tokens * width)),
        name="text_kv",
    )(text.reshape(tokens, width), w_kv.reshape(2, total, width))


def cross_mlp(me, chunks, modulation, k, v_t, w_query, w_out_cross, w_in, w_out, base, y, videos):
    count, quarter, width = chunks[0].shape
    tokens = 4 * quarter
    heads, dim, all_text = v_t.shape
    text = all_text // videos
    total = heads * dim
    hidden = w_in.shape[1]
    tile = 512
    steps = hidden // tile
    in_specs = [pl.BlockSpec((None, quarter, width), lambda v, s, me: (v, 0, 0))] * 4 + [
        pl.BlockSpec((None, 6, width), lambda v, s, me: (base + v, 0, 0)),
        pl.BlockSpec((heads, text, k.shape[2]), lambda v, s, me: (0, base + v, 0)),
        pl.BlockSpec((heads, dim, text), lambda v, s, me: (0, 0, base + v)),
        pl.BlockSpec(memory_space=pl.ANY),
        pl.BlockSpec(memory_space=pl.ANY),
        pl.BlockSpec((width, tile), lambda v, s, me: (0, s)),
        pl.BlockSpec((tile, width), lambda v, s, me: (s, 0)),
    ]
    args = [me, *chunks, modulation, k, v_t, w_query.reshape(total, width), w_out_cross.reshape(total, width), w_in, w_out]
    aliases = {}
    if y is not None:
        in_specs.append(pl.BlockSpec(memory_space=pl.ANY))
        aliases = {len(args): 0}
        args.append(y)
    spec = pltpu.PrefetchScalarGridSpec(
        num_scalar_prefetch=1,
        grid=(count, steps),
        in_specs=in_specs,
        out_specs=pl.BlockSpec((None, None, tokens, width), lambda v, s, me: (base + v, 0, 0, 0)),
        scratch_shapes=[
            pltpu.VMEM((heads, 128, tokens), BF16),
            pltpu.VMEM((total, tokens), BF16),
            pltpu.VMEM((tokens, width), BF16),
            pltpu.VMEM((tokens, width), BF16),
            pltpu.VMEM((tokens, width), F32),
            pltpu.VMEM((total, width), BF16),
            pltpu.VMEM((total, width), BF16),
            pltpu.VMEM((text, 512), F32),
            pltpu.VMEM((text, 512), F32),
            pltpu.VMEM((text, 512), BF16),
            pltpu.VMEM((text, 512), BF16),
            pltpu.SemaphoreType.DMA((2,)),
        ],
    )
    return pl.pallas_call(
        functools.partial(cross_mlp_kernel, heads=heads, dim=dim),
        grid_spec=spec,
        out_shape=jax.ShapeDtypeStruct((videos, 1, tokens, width), BF16),
        input_output_aliases=aliases,
        compiler_params=params(),
        cost_estimate=cost(count * 4 * tokens * width * (hidden + total) + 4 * tokens * text * total, 4 * (width * hidden + total * width + tokens * width)),
        name="cross_mlp",
    )(*args)


def swap(parts, devices):
    return [parts[0]] + [lax.ppermute(parts[d], 'sp', [(i, i ^ d) for i in range(devices)]) for d in range(1, devices)]


def solution(mesh):
    act_spec = P('dp', 'sp', None, None)
    row_spec = P('dp', None, None)
    rep_two = P(None, None)
    rep_three = P(None, None, None)
    rep_four = P(None, None, None, None)
    in_specs = (act_spec, row_spec, row_spec, rep_two, rep_four, rep_three, rep_four, rep_three, rep_three, rep_four, rep_three, rep_two, rep_two)
    devices = mesh.shape['sp']

    def local_block(latents, text_ctx, modulation, pos_temporal, w_qkv_spatial, w_out_spatial, w_qkv_temporal, w_out_temporal, w_query_cross, w_kv_cross, w_out_cross, w_mlp_in, w_mlp_out):
        videos = latents.shape[0]
        me = lax.axis_index('sp').astype(jnp.int32).reshape(1)
        bases = range(0, videos, 2)
        by_patch = [swap(spatial(me, latents, modulation, w_qkv_spatial, w_out_spatial, b, 2, 4), devices) for b in bases]
        k, v_t = text_kv(text_ctx, w_kv_cross, 4)
        by_frame = [swap(temporal(me, by_patch[i], modulation, pos_temporal, w_qkv_temporal, w_out_temporal, b, 4), devices) for i, b in enumerate(bases)]
        y = None
        for i, b in enumerate(bases):
            y = cross_mlp(me, by_frame[i], modulation, k, v_t, w_query_cross, w_out_cross, w_mlp_in, w_mlp_out, b, y, videos)
        return y

    return jax.shard_map(local_block, mesh=mesh, in_specs=in_specs, out_specs=act_spec, check_vma=False)
```

```python
import functools

import jax
import jax.numpy as jnp
from jax import lax
from jax.experimental import pallas as pl
from jax.experimental.pallas import tpu as pltpu
from jax.sharding import PartitionSpec as P

LN_EPS = 1e-6
LOG2E = 1.4426950408889634
VMEM_LIMIT = 67043328
NT = (((1,), (1,)), ((), ()))
TN = (((0,), (0,)), ((), ()))
F32 = jnp.float32
BF16 = jnp.bfloat16


def dot(lhs, rhs, dims=(((1,), (0,)), ((), ()))):
    return lax.dot_general(lhs, rhs, dims, preferred_element_type=F32)


def normed_rows(rows, shift, scale):
    rows = rows.astype(F32)
    centered = rows - jnp.mean(rows, axis=-1, keepdims=True)
    unit = centered * lax.rsqrt(jnp.mean(centered * centered, axis=-1, keepdims=True) + LN_EPS)
    return (unit * (1.0 + scale) + shift).astype(BF16)


def resident(shape):
    return pl.BlockSpec(shape, lambda *_: (0,) * len(shape), pipeline_mode=pl.Buffered(1))


def project_heads(w_ref, acts, q_s, k_s, v_s, heads, dim, cols):
    chunk = cols.stop - cols.start
    part = acts[cols, :]
    q_s[:, :dim, cols] = dot(w_ref[0], part, NT).reshape(heads, dim, chunk).astype(BF16)
    v_s[:, :, cols] = dot(w_ref[2], part, NT).reshape(heads, dim, chunk).astype(BF16)
    k_t = dot(w_ref[1], part, NT)
    for h in range(heads):
        k_s[h, cols, :dim] = k_t[h * dim:(h + 1) * dim].T.astype(BF16)


def attend_heads(q, k, v, out, scores, probs, base, row, scale, count, block):
    tokens, keys, dim = out.shape[1], k.shape[1], v.shape[1]
    chunk = min(256, keys)
    blocks = [(h, c) for c in range(tokens // block) for h in range(count)]
    tops, mixed = {}, {}

    def score(n):
        h, c = blocks[n]
        top = None
        for r in range(0, keys, chunk):
            s = dot(k[base + h, r:r + chunk, :], q[base + h, :, c * block:(c + 1) * block])
            scores[n % 2][r:r + chunk, :] = s
            part = jnp.max(s.reshape(chunk // 8, 8, block), axis=0)
            top = part if top is None else jnp.maximum(top, part)
        tops[n] = jnp.max(top, axis=0, keepdims=True)

    def mix(n):
        h, c = blocks[n]
        total = None
        for r in range(0, keys, chunk):
            p = jnp.exp2((scores[n % 2][r:r + chunk, :] - tops[n]) * scale)
            part = jnp.sum(p.reshape(chunk // 8, 8, block), axis=0)
            total = part if total is None else total + part
            probs[n % 2][r:r + chunk, :] = p.astype(BF16)
        mixed[h] = dot(v[base + h], probs[n % 2][...]) / jnp.sum(total, axis=0, keepdims=True)
        if h == count - 1:
            out[pl.ds(row, count * dim), c * block:(c + 1) * block] = jnp.concatenate([mixed[i] for i in range(count)], axis=0).astype(BF16)

    score(0)
    for n in range(len(blocks)):
        if n + 1 < len(blocks):
            score(n + 1)
        mix(n)


def gelu(x):
    return x * (0.5 + 0.5 * jnp.tanh(x * (0.7978845608028654 + 0.7978845608028654 * 0.044715 * (x * x))))


def spatial_kernel(me_ref, x_ref, mod_ref, w_ref, wo_hbm, o0, o1, o2, o3, u_s, q_s, k_s, v_s, a_s, wo_s, s0, s1, p0, p1, sem, *, heads, dim):
    v, g = pl.program_id(0), pl.program_id(1)
    tokens = x_ref.shape[0]
    quarter = tokens // 4
    halves = (slice(0, tokens // 2), slice(tokens // 2, tokens))
    wo_copy = pltpu.make_async_copy(wo_hbm, wo_s, sem)
    scale = dim ** -0.5 * LOG2E

    @pl.when((v == 0) & (g == 0))
    def _():
        q_s[:, dim:, :] = jnp.zeros((heads, q_s.shape[1] - dim, tokens), BF16)
        k_s[:, :, dim:] = jnp.zeros((heads, tokens, k_s.shape[2] - dim), BF16)

    @pl.when(g == 0)
    def _():
        for rows in halves:
            u_s[rows, :] = normed_rows(x_ref[rows, :], mod_ref[0:1, :], mod_ref[1:2, :])
            project_heads(w_ref, u_s, q_s, k_s, v_s, heads, dim, rows)

    @pl.when(g > 0)
    def _():
        for rows in halves:
            project_heads(w_ref, u_s, q_s, k_s, v_s, heads, dim, rows)

    @pl.when((v == 0) & (g == 1))
    def _():
        wo_copy.start()

    def pair(i, carry):
        row = pl.multiple_of((g * heads + 2 * i) * dim, 2 * dim)
        attend_heads(q_s, k_s, v_s, a_s, (s0, s1), (p0, p1), 2 * i, row, scale, 2, 512)
        return carry

    lax.fori_loop(0, heads // 2, pair, 0)

    @pl.when((v == 0) & (g == pl.num_programs(1) - 1))
    def _():
        wo_copy.wait()

    @pl.when(g == pl.num_programs(1) - 1)
    def _():
        for d, o_ref in enumerate((o0, o1, o2, o3)):
            rows = pl.ds(pl.multiple_of(jnp.bitwise_xor(me_ref[0], d) * quarter, quarter), quarter)
            branch = dot(a_s[:, rows], wo_s[...], TN)
            o_ref[...] = (x_ref[rows, :].astype(F32) + mod_ref[2:3, :] * branch).astype(BF16)


def attend_frames(q_s, k_s, v_s, h, cols, quarter, scale):
    part = lambda ref, t: ref[h, :, t * quarter + cols:t * quarter + cols + 128].astype(F32)
    k = [part(k_s, t) for t in range(4)]
    v = [part(v_s, t) for t in range(4)]
    outs = []
    for t in range(4):
        q = part(q_s, t)
        s = [jnp.sum(q * one, axis=0, keepdims=True) for one in k]
        top = jnp.maximum(jnp.maximum(s[0], s[1]), jnp.maximum(s[2], s[3]))
        p = [jnp.exp2((one - top) * scale) for one in s]
        inv = 1.0 / (p[0] + p[1] + p[2] + p[3])
        p = [(one * inv).astype(BF16).astype(F32) for one in p]
        outs.append(p[0] * v[0] + p[1] * v[1] + p[2] * v[2] + p[3] * v[3])
    return outs


def temporal_kernel(me_ref, x0, x1, x2, x3, mod_ref, pos_ref, w_ref, wo_hbm, o0, o1, o2, o3, z_s, qa, ka, va, qb, kb, vb, a_s, wo_s, sem, *, heads, dim):
    v, g = pl.program_id(0), pl.program_id(1)
    quarter = x0.shape[0]
    frames = (x0, x1, x2, x3)
    group = heads * dim
    wo_copy = pltpu.make_async_copy(wo_hbm, wo_s, sem)
    scale = dim ** -0.5 * LOG2E

    def shift(d):
        pos = pos_ref[pl.ds(jnp.bitwise_xor(me_ref[0], d), 1), :]
        z_s[d * quarter:(d + 1) * quarter, :] = (frames[d][...].astype(F32) + pos).astype(BF16)

    def project(half, dsts, tokens):
        for j, dst in enumerate(dsts):
            part = dot(w_ref[j, half * group:(half + 1) * group, :], z_s[tokens, :], NT)
            dst[:, :, tokens] = part.reshape(heads, dim, 2 * quarter).astype(BF16)

    def attend(srcs, index):
        def pair(i, carry):
            rows = pl.ds(pl.multiple_of(index * group + 2 * i * dim, 2 * dim), 2 * dim)
            for cols in range(0, quarter, 128):
                first = attend_frames(*srcs, 2 * i, cols, quarter, scale)
                second = attend_frames(*srcs, 2 * i + 1, cols, quarter, scale)
                for t in range(4):
                    out = jnp.concatenate([first[t], second[t]], axis=0)
                    a_s[rows, t * quarter + cols:t * quarter + cols + 128] = out.astype(BF16)
            return carry

        lax.fori_loop(0, heads // 2, pair, 0)

    halves = (slice(0, 2 * quarter), slice(2 * quarter, 4 * quarter))
    first, second = (qa, ka, va), (qb, kb, vb)

    @pl.when(g == 0)
    def _():
        for d in range(4):
            shift(d)

    for tokens in halves:
        project(0, first, tokens)
        project(1, second, tokens)
    attend(first, 2 * g)
    attend(second, 2 * g + 1)

    @pl.when((v == 0) & (g == 0))
    def _():
        wo_copy.start()

    @pl.when((v == 0) & (g == pl.num_programs(1) - 1))
    def _():
        wo_copy.wait()

    @pl.when(g == pl.num_programs(1) - 1)
    def _():
        for d, (x, o_ref) in enumerate(zip(frames, (o0, o1, o2, o3))):
            branch = dot(a_s[:, d * quarter:(d + 1) * quarter], wo_s[...], TN)
            o_ref[...] = (x[...].astype(F32) + mod_ref[2:3, :] * branch).astype(BF16)


def text_kernel(t_ref, w_ref, k_ref, v_ref, *, heads, dim):
    tokens = t_ref.shape[0]
    k_t = dot(w_ref[0], t_ref[...], NT)
    v_ref[...] = dot(w_ref[1], t_ref[...], NT).reshape(heads, dim, tokens).astype(BF16)
    k_ref[:, :, dim:] = jnp.zeros((heads, tokens, k_ref.shape[2] - dim), BF16)
    for h in range(heads):
        k_ref[h, :, :dim] = k_t[h * dim:(h + 1) * dim].T.astype(BF16)


def cross_mlp_kernel(me_ref, x0, x1, x2, x3, mod_ref, k_ref, v_ref, wq_hbm, wo_hbm, w_in, w_out, *rest, heads, dim):
    y_ref, q_s, a_s, h_s, u_s, acc_s, wq_s, wo_s, s0, s1, p0, p1, sems = rest[-13:]
    v, step = pl.program_id(0), pl.program_id(1)
    quarter = x0.shape[0]
    tokens = 4 * quarter
    scale = dim ** -0.5 * LOG2E

    @pl.when(step == 0)
    def _():
        acc_s[...] = jnp.zeros_like(acc_s)

        @pl.when(v == 0)
        def _():
            pltpu.make_async_copy(wq_hbm, wq_s, sems.at[0]).start()
            pltpu.make_async_copy(wq_hbm, wq_s, sems.at[0]).wait()
            pltpu.make_async_copy(wo_hbm, wo_s, sems.at[1]).start()

        for d, x in enumerate((x0, x1, x2, x3)):
            cols = slice(d * quarter, (d + 1) * quarter)
            q_s[:, :dim, cols] = dot(wq_s[...], x[...], NT).reshape(heads, dim, quarter).astype(BF16)
        q_s[:, dim:, :] = jnp.zeros((heads, q_s.shape[1] - dim, tokens), BF16)

        def four(i, carry):
            row = pl.multiple_of(4 * i * dim, 4 * dim)
            attend_heads(q_s, k_ref, v_ref, a_s, (s0, s1), (p0, p1), 4 * i, row, scale, 4, 512)
            return carry

        lax.fori_loop(0, heads // 4, four, 0)

        @pl.when(v == 0)
        def _():
            pltpu.make_async_copy(wo_hbm, wo_s, sems.at[1]).wait()

        for d, x in enumerate((x0, x1, x2, x3)):
            rows = slice(d * quarter, (d + 1) * quarter)
            branch = dot(a_s[:, rows], wo_s[...], TN)
            after = (x[...].astype(F32) + branch).astype(BF16)
            h_s[rows, :] = after
            u_s[rows, :] = normed_rows(after, mod_ref[3:4, :], mod_ref[4:5, :])

    hidden = gelu(dot(u_s[...], w_in[...])).astype(BF16)
    acc_s[...] += dot(hidden, w_out[...])

    @pl.when(step == pl.num_programs(1) - 1)
    def _():
        for d in range(4):
            rows = slice(d * quarter, (d + 1) * quarter)
            dst = pl.ds(pl.multiple_of(jnp.bitwise_xor(me_ref[0], d) * quarter, quarter), quarter)
            y_ref[dst, :] = (h_s[rows, :].astype(F32) + mod_ref[5:6, :] * acc_s[rows, :]).astype(BF16)


def cost(flops, nbytes, exps=0):
    return pl.CostEstimate(flops=int(flops), bytes_accessed=int(nbytes), transcendentals=int(exps))


def params(axes=2):
    return pltpu.CompilerParams(dimension_semantics=("arbitrary",) * axes, vmem_limit_bytes=VMEM_LIMIT)


def spatial(me, latents, modulation, w_qkv, w_out, base, videos, heads):
    tokens, width = latents.shape[2:]
    dim = w_qkv.shape[2]
    total = w_qkv.shape[1] * dim
    group, quarter = heads * dim, tokens // 4
    spec = pltpu.PrefetchScalarGridSpec(
        num_scalar_prefetch=1,
        grid=(videos, w_qkv.shape[1] // heads),
        in_specs=[
            pl.BlockSpec((None, None, tokens, width), lambda v, g, me: (base + v, 0, 0, 0)),
            pl.BlockSpec((None, 6, width), lambda v, g, me: (base + v, 0, 0)),
            pl.BlockSpec((3, group, width), lambda v, g, me: (0, g, 0)),
            pl.BlockSpec(memory_space=pl.ANY),
        ],
        out_specs=[pl.BlockSpec((None, quarter, width), lambda v, g, me: (v, 0, 0))] * 4,
        scratch_shapes=[
            pltpu.VMEM((tokens, width), BF16),
            pltpu.VMEM((heads, 128, tokens), BF16),
            pltpu.VMEM((heads, tokens, 128), BF16),
            pltpu.VMEM((heads, dim, tokens), BF16),
            pltpu.VMEM((total, tokens), BF16),
            pltpu.VMEM((total, width), BF16),
            pltpu.VMEM((tokens, 512), F32),
            pltpu.VMEM((tokens, 512), F32),
            pltpu.VMEM((tokens, 512), BF16),
            pltpu.VMEM((tokens, 512), BF16),
            pltpu.SemaphoreType.DMA,
        ],
    )
    return pl.pallas_call(
        functools.partial(spatial_kernel, heads=heads, dim=dim),
        grid_spec=spec,
        out_shape=[jax.ShapeDtypeStruct((videos, quarter, width), BF16)] * 4,
        compiler_params=params(),
        cost_estimate=cost(videos * (8 * tokens * width * total + 4 * tokens * tokens * total), 2 * (4 * total * width + 2 * videos * tokens * width)),
        name="spatial",
    )(me, latents, modulation, w_qkv.reshape(3, total, width), w_out.reshape(total, width))


def temporal(me, frames, modulation, pos, w_qkv, w_out, base, heads):
    videos, quarter, width = frames[0].shape
    tokens = 4 * quarter
    dim = w_qkv.shape[2]
    total = w_qkv.shape[1] * dim
    group = heads * dim
    spec = pltpu.PrefetchScalarGridSpec(
        num_scalar_prefetch=1,
        grid=(videos, w_qkv.shape[1] // (2 * heads)),
        in_specs=[pl.BlockSpec((None, quarter, width), lambda v, g, me: (v, 0, 0))] * 4 + [
            pl.BlockSpec((None, 6, width), lambda v, g, me: (base + v, 0, 0)),
            resident(pos.shape),
            pl.BlockSpec((3, 2 * group, width), lambda v, g, me: (0, g, 0)),
            pl.BlockSpec(memory_space=pl.ANY),
        ],
        out_specs=[pl.BlockSpec((None, quarter, width), lambda v, g, me: (v, 0, 0))] * 4,
        scratch_shapes=[pltpu.VMEM((tokens, width), BF16)] + [pltpu.VMEM((heads, dim, tokens), BF16)] * 6 + [
            pltpu.VMEM((total, tokens), BF16),
            pltpu.VMEM((total, width), BF16),
            pltpu.SemaphoreType.DMA,
        ],
    )
    return pl.pallas_call(
        functools.partial(temporal_kernel, heads=heads, dim=dim),
        grid_spec=spec,
        out_shape=[jax.ShapeDtypeStruct((videos, quarter, width), BF16)] * 4,
        compiler_params=params(),
        cost_estimate=cost(videos * 8 * tokens * width * total, 2 * (4 * total * width + 2 * videos * tokens * width)),
        name="temporal",
    )(me, *frames, modulation, pos, w_qkv.reshape(3, total, width), w_out.reshape(total, width))


def text_kv(text, w_kv, heads, part, parts):
    videos, length, width = text.shape
    dim = w_kv.shape[2]
    count = w_kv.shape[1]
    total = count * dim
    tokens = videos * length // parts
    return pl.pallas_call(
        functools.partial(text_kernel, heads=heads, dim=dim),
        grid=(count // heads,),
        in_specs=[pl.BlockSpec((tokens, width), lambda g: (part, 0), pipeline_mode=pl.Buffered(1)), pl.BlockSpec((2, heads * dim, width), lambda g: (0, g, 0))],
        out_specs=[pl.BlockSpec((heads, tokens, 128), lambda g: (g, 0, 0)), pl.BlockSpec((heads, dim, tokens), lambda g: (g, 0, 0))],
        out_shape=[jax.ShapeDtypeStruct((count, tokens, 128), BF16), jax.ShapeDtypeStruct((count, dim, tokens), BF16)],
        compiler_params=params(1),
        cost_estimate=cost(4 * tokens * width * total, 2 * (2 * total * width + 3 * tokens * width)),
        name="text_kv",
    )(text.reshape(videos * length, width), w_kv.reshape(2, total, width))


def cross_mlp(me, chunks, modulation, k, v_t, w_query, w_out_cross, w_in, w_out, base, y, videos):
    count, quarter, width = chunks[0].shape
    tokens = 4 * quarter
    heads, dim, all_text = v_t.shape
    text = all_text // count
    total = heads * dim
    hidden = w_in.shape[1]
    tile = 512
    steps = hidden // tile
    in_specs = [pl.BlockSpec((None, quarter, width), lambda v, s, me: (v, 0, 0))] * 4 + [
        pl.BlockSpec((None, 6, width), lambda v, s, me: (base + v, 0, 0)),
        pl.BlockSpec((heads, text, k.shape[2]), lambda v, s, me: (0, v, 0)),
        pl.BlockSpec((heads, dim, text), lambda v, s, me: (0, 0, v)),
        pl.BlockSpec(memory_space=pl.ANY),
        pl.BlockSpec(memory_space=pl.ANY),
        pl.BlockSpec((width, tile), lambda v, s, me: (0, s)),
        pl.BlockSpec((tile, width), lambda v, s, me: (s, 0)),
    ]
    args = [me, *chunks, modulation, k, v_t, w_query.reshape(total, width), w_out_cross.reshape(total, width), w_in, w_out]
    aliases = {}
    if y is not None:
        in_specs.append(pl.BlockSpec(memory_space=pl.ANY))
        aliases = {len(args): 0}
        args.append(y)
    spec = pltpu.PrefetchScalarGridSpec(
        num_scalar_prefetch=1,
        grid=(count, steps),
        in_specs=in_specs,
        out_specs=pl.BlockSpec((None, None, tokens, width), lambda v, s, me: (base + v, 0, 0, 0)),
        scratch_shapes=[
            pltpu.VMEM((heads, 128, tokens), BF16),
            pltpu.VMEM((total, tokens), BF16),
            pltpu.VMEM((tokens, width), BF16),
            pltpu.VMEM((tokens, width), BF16),
            pltpu.VMEM((tokens, width), F32),
            pltpu.VMEM((total, width), BF16),
            pltpu.VMEM((total, width), BF16),
            pltpu.VMEM((text, 512), F32),
            pltpu.VMEM((text, 512), F32),
            pltpu.VMEM((text, 512), BF16),
            pltpu.VMEM((text, 512), BF16),
            pltpu.SemaphoreType.DMA((2,)),
        ],
    )
    return pl.pallas_call(
        functools.partial(cross_mlp_kernel, heads=heads, dim=dim),
        grid_spec=spec,
        out_shape=jax.ShapeDtypeStruct((videos, 1, tokens, width), BF16),
        input_output_aliases=aliases,
        compiler_params=params(),
        cost_estimate=cost(count * 4 * tokens * width * (hidden + total) + 4 * tokens * text * total, 4 * (width * hidden + total * width + tokens * width)),
        name="cross_mlp",
    )(*args)


def swap(parts, devices):
    return [parts[0]] + [lax.ppermute(parts[d], 'sp', [(i, i ^ d) for i in range(devices)]) for d in range(1, devices)]


def solution(mesh):
    act_spec = P('dp', 'sp', None, None)
    row_spec = P('dp', None, None)
    rep_two = P(None, None)
    rep_three = P(None, None, None)
    rep_four = P(None, None, None, None)
    in_specs = (act_spec, row_spec, row_spec, rep_two, rep_four, rep_three, rep_four, rep_three, rep_three, rep_four, rep_three, rep_two, rep_two)
    devices = mesh.shape['sp']

    def local_block(latents, text_ctx, modulation, pos_temporal, w_qkv_spatial, w_out_spatial, w_qkv_temporal, w_out_temporal, w_query_cross, w_kv_cross, w_out_cross, w_mlp_in, w_mlp_out):
        videos = latents.shape[0]
        me = lax.axis_index('sp').astype(jnp.int32).reshape(1)
        bases = range(0, videos, 2)
        by_patch = [swap(spatial(me, latents, modulation, w_qkv_spatial, w_out_spatial, b, 2, 4), devices) for b in bases]
        text, _ = lax.optimization_barrier((text_ctx, by_patch[-1][0]))
        context = [text_kv(text, w_kv_cross, 4, 0, 2)]
        first, _ = lax.optimization_barrier((by_patch[0], context[0][1]))
        by_patch = [first] + by_patch[1:]
        mixed = [temporal(me, by_patch[i], modulation, pos_temporal, w_qkv_temporal, w_out_temporal, b, 4) for i, b in enumerate(bases)]
        by_frame = [swap(parts, devices) for parts in mixed]
        text, _ = lax.optimization_barrier((text_ctx, mixed[-1][0]))
        context.append(text_kv(text, w_kv_cross, 4, 1, 2))
        y = None
        for i, b in enumerate(bases):
            y = cross_mlp(me, by_frame[i], modulation, *context[i], w_query_cross, w_out_cross, w_mlp_in, w_mlp_out, b, y, videos)
        return y

    return jax.shard_map(local_block, mesh=mesh, in_specs=in_specs, out_specs=act_spec, check_vma=False)
```
